256 devices in a mesh: row: 4 (over x_lo, core), col: 64 (over y, z, x_hi).
Axes of the slice: x: 4 (x_hi: 2, x_lo: 2; x = x_hi * 2 + x_lo), y: 4, z: 8, core: 2. Of those that a mesh axis runs over, the one named last changes fastest.
Arguments:
- old_table: float32 [64, 4096, 128], P('col', 'row'), may hold values from -1 to 1
- old_blocks: int32 [64, 32], P('col', 'row'), may hold values from 0 to 31, as said below
- new_blocks: int32 [64, 32], P('col', 'row'), may hold values from 0 to 31, as said below
- bag_row_index: int32 [4096, 64, 64], P(None, 'col'), may hold values from 0 to 4095
- bag_length: int32 [4096, 64], P(None, 'col'), may hold values from 1 to 64
- dense: bfloat16 [4096, 128], P(('row', 'col')), may hold values from -6 to 6
- w_first: bfloat16 [2208, 1024], replicated, may hold values from -0.25 to 0.25
- w_second: bfloat16 [1024, 1024], replicated, may hold values from -0.25 to 0.25
- w_out: bfloat16 [1024], replicated, may hold values from -0.75 to 0.75
Outputs:
- logits: float32 [4096], P(('row', 'col'))
- new_tables: float32 [64, 4096, 128], P('col', 'row')
The draws below stay inside these ranges and needn't reach their ends.
Inputs may be any that keep to these rules, and one draw needn't show every extreme that they name: `old_blocks`: for each table a permutation of the blocks; row device r holds positions r * 8 to (r + 1) * 8 - 1. For each table a permutation of the blocks; for every ordered pair of row devices, exactly 2 of the blocks that the first holds in old_blocks lie on the second in new_blocks.
All inputs are finite; a program needn't handle non-finite values.
Results may differ from the reference program's by a relative error of at most 0.0069.
Values sent between devices are 32-bit elements; how exact they have to be, the bound alone decides.
No kernel may reach another device: no remote copies, remote signals or barrier semaphores. Data moves between devices by JAX's collectives and lax.ppermute only.
A program may use at most 64 MiB of HBM per device.

```python
import math
import jax
import jax.numpy as jnp
import numpy as np
from jax import lax

EMBED_WIDTH = 128
H = 1024
BLK = 128
L = 64
SLOTS = 8
NTAB = 64
NBLK = 32
MOVE = 2
TROWS = 4096
SAMPLES = 4096
F = 2208
N_ROW = 4


def layout_pair(key):
    table_keys = jax.random.split(jax.random.fold_in(key, 7), NTAB)

    def one_table(table_key):
        first_key, second_key, third_key = jax.random.split(table_key, 3)
        before = jax.random.permutation(first_key, NBLK).astype(jnp.int32)
        shuffled = jax.vmap(lambda inner: jax.random.permutation(inner, SLOTS))(jax.random.split(second_key, N_ROW))
        anchor = jnp.arange(N_ROW, dtype=jnp.int32)[:, None] * SLOTS + shuffled.astype(jnp.int32)
        offered = anchor.reshape(N_ROW, N_ROW, MOVE).transpose(1, 0, 2).reshape(N_ROW, SLOTS)
        placing = jax.vmap(lambda inner: jax.random.permutation(inner, SLOTS))(jax.random.split(third_key, N_ROW))
        taken = jnp.take_along_axis(offered, placing.astype(jnp.int32), axis=1).reshape(NBLK)
        after = jnp.take(before, taken, axis=0)
        return (before, after)
    return jax.vmap(one_table)(table_keys)


def draw_old_blocks(key, part):
    return layout_pair(key)[0]


def draw_new_blocks(key, part):
    return layout_pair(key)[1]


def set_ends(array, stream_key, least, top_value):
    longest = array.shape.index(max(array.shape))
    spots = []
    for shift in (0, 1):
        where = [jax.random.randint(jax.random.fold_in(stream_key, axis), (), 0, length) for axis, length in enumerate(array.shape)]
        where[longest] = (where[longest] + shift) % array.shape[longest]
        spots.append(tuple(where))
    return array.at[spots[0]].set(least).at[spots[1]].set(top_value)


def shard_levels(own_key, extent, pieces, least, top_value):
    loudness = 1.0
    for axis_at, parts in pieces:
        steps = jax.random.uniform(jax.random.fold_in(jax.random.fold_in(own_key, 6), axis_at), (parts,), jnp.float32, least / len(pieces), top_value / len(pieces))
        loudness = loudness * jnp.repeat(jnp.exp(steps), extent[axis_at] // parts).reshape((-1,) + (1,) * (len(extent) - 1 - axis_at))
    return loudness


def cumulative_ranks(amount, lean):
    loads = [(1 << 20) // math.isqrt(rank ** lean) + 1 for rank in range(1, amount + 1)]
    deviation = 1 + sum(loads) // (1 << 30)
    return np.cumsum(np.array([max(1, weight // deviation) for weight in loads]))


def ranked_ids(rng, extent, amount, slope):
    grid = cumulative_ranks(amount, slope)
    lot = jax.random.randint(jax.random.fold_in(rng, 1), extent, 0, int(grid[amount - 1]))
    grade = jnp.searchsorted(jnp.asarray(grid, jnp.int32), lot, side="right")
    return jax.random.permutation(jax.random.fold_in(rng, 2), amount)[grade].astype(jnp.int32)


def scatter_about(key, extent, width, reach, cuts=(), held_as=jnp.bfloat16):
    entries = jax.random.normal(key, extent, jnp.float32) * width
    if len(cuts) > 0:
        entries = shard_levels(key, extent, cuts, -0.22, 0.18) * entries
    return jnp.clip(entries, min=-reach, max=reach).astype(held_as)


def setup_inputs(seed: int = 0) -> dict:
    arg_keys = jax.random.split(jax.random.key(seed), 10)
    return {
        "old_table": scatter_about(arg_keys[0], (NTAB, TROWS, EMBED_WIDTH), 0.125, 1.0, ((0, 64), (1, 4)), jnp.float32),
        "old_blocks": draw_old_blocks(jax.random.fold_in(arg_keys[9], 71), 0),
        "new_blocks": draw_new_blocks(jax.random.fold_in(arg_keys[9], 71), 0),
        "bag_row_index": set_ends(ranked_ids(arg_keys[3], (SAMPLES, NTAB, L), TROWS, 2), jax.random.fold_in(arg_keys[3], 3), 0, TROWS - 1).astype(jnp.int32),
        "bag_length": set_ends(jax.random.randint(arg_keys[4], (SAMPLES, NTAB), 1, L + 1), jax.random.fold_in(arg_keys[4], 1), 1, L).astype(jnp.int32),
        "dense": scatter_about(arg_keys[5], (SAMPLES, EMBED_WIDTH), 1.0, 6.0, ((0, 256),)),
        "w_first": scatter_about(arg_keys[6], (F, H), (F // 4) ** -0.5, 0.25),
        "w_second": scatter_about(arg_keys[7], (H, H), (H // 2) ** -0.5, 0.25),
        "w_out": scatter_about(arg_keys[8], (H,), (H // 16) ** -0.5, 0.75),
    }


strict_precision = lax.Precision.HIGHEST


def pool_table(operands):
    table_rows, indices, weights = operands
    return jnp.sum(jnp.take(table_rows, indices, axis=0) * weights[:, :, None], axis=1)


def reference(old_table, old_blocks, new_blocks, bag_row_index, bag_length, dense, w_first, w_second, w_out):
    stored = old_table.reshape(NTAB, NBLK, BLK, EMBED_WIDTH)
    tables = jnp.arange(NTAB, dtype=jnp.int32)[:, None]
    logical = jnp.zeros_like(stored).at[tables, old_blocks.astype(jnp.int32)].set(stored)
    new_tables = logical[tables, new_blocks.astype(jnp.int32)].reshape(NTAB, TROWS, EMBED_WIDTH)
    is_live = (jnp.arange(L, dtype=jnp.int32)[None, None, :] < bag_length[:, :, None]).astype(jnp.float32)
    pooled = lax.map(pool_table, (logical.reshape(NTAB, TROWS, EMBED_WIDTH), jnp.transpose(bag_row_index, (1, 0, 2)), jnp.transpose(is_live, (1, 0, 2))))
    pooled = jnp.transpose(pooled, (1, 0, 2))
    dense_wide = dense.astype(jnp.float32)
    stacked_vectors = jnp.concatenate([dense_wide[:, None, :], pooled], axis=1)
    interaction_matrix = jnp.einsum("cxp,cfp->cxf", stacked_vectors, stacked_vectors, precision=strict_precision) * (EMBED_WIDTH ** -0.5)
    upper_index, lower_index = np.triu_indices(NTAB + 1, 1)
    crossed = interaction_matrix[:, upper_index, lower_index]
    joined = jnp.concatenate([dense_wide, crossed], axis=1).astype(jnp.bfloat16)
    hidden_one = jnp.maximum(jnp.dot(joined, w_first, preferred_element_type=jnp.float32), 0.0).astype(jnp.bfloat16)
    hidden_two = jnp.maximum(jnp.dot(hidden_one, w_second, preferred_element_type=jnp.float32), 0.0).astype(jnp.bfloat16)
    logits = jnp.dot(hidden_two, w_out, preferred_element_type=jnp.float32)
    return logits, new_tables
```

```python
import functools
import math

import jax
import jax.numpy as jnp
import numpy as np
from jax import lax
from jax.experimental import pallas as pl
from jax.experimental.pallas import tpu as pltpu
from jax.sharding import PartitionSpec as P

BLK = 128
BF16 = jnp.bfloat16
F32 = jnp.float32


def halves(x):
    top = x.astype(BF16)
    rest = (x - top.astype(F32)).astype(BF16)
    return top, rest


def count_kernel(rank_ref, index_ref, length_ref, counts_ref, block_key, offset_key, staged):
    bag = index_ref.shape[0]
    group = index_ref.shape[1]
    half = group // 2
    blocks = counts_ref.shape[0]
    pitch = staged.shape[0] // group
    place = lax.broadcasted_iota(jnp.int32, (bag, group), 0)
    rows = jnp.where(place < length_ref[...], index_ref[...], -1)
    rows = jnp.transpose(rows, (1, 0))
    block = rows // BLK
    block = jnp.where(rows < 0, -1, lax.shift_right_arithmetic(rows, 7))
    offset = rows & (BLK - 1)
    second = jnp.where(block[half:] < 0, -1, block[half:] + blocks)
    block_key[...] = jnp.concatenate([block[:half], second], axis=1)
    offset_key[...] = jnp.concatenate([offset[:half], offset[half:]], axis=1)
    block_order = lax.broadcasted_iota(jnp.int32, (2 * blocks, 2 * bag), 0)
    offset_order = lax.broadcasted_iota(jnp.int32, (BLK, 2 * bag), 0)

    def pair(n):
        in_block = jnp.where(block_key[pl.ds(n, 1), :] == block_order, 1.0, 0.0).astype(BF16)
        at_offset = jnp.where(offset_key[pl.ds(n, 1), :] == offset_order, 1.0, 0.0).astype(BF16)
        found = lax.dot_general(
            in_block, at_offset, (((1,), (1,)), ((), ())), preferred_element_type=F32
        )
        staged[pl.ds(pl.multiple_of(n * pitch, 8), blocks), :] = found[:blocks]
        staged[pl.ds(pl.multiple_of((n + half) * pitch, 8), blocks), :] = found[blocks:]

    def some(step, carry):
        for k in range(8):
            pair(step * 8 + k)
        return carry

    lax.fori_loop(0, half // 8, some, 0)
    for b in range(blocks):
        counts_ref[b] = staged[pl.ds(b, group, stride=pitch), :].astype(BF16)


def count_bags(rank, index, length, share, blocks):
    bag = index.shape[0]
    group = 128
    steps = share // group
    return pl.pallas_call(
        count_kernel,
        grid_spec=pltpu.PrefetchScalarGridSpec(
            num_scalar_prefetch=1,
            grid=(steps,),
            in_specs=[
                pl.BlockSpec((bag, group), lambda g, rank: (0, rank[0] * steps + g)),
                pl.BlockSpec((1, group), lambda g, rank: (0, rank[0] * steps + g)),
            ],
            out_specs=pl.BlockSpec((blocks, group, BLK), lambda g, rank: (0, g, 0)),
            scratch_shapes=[
                pltpu.VMEM((group // 2, 2 * bag), jnp.int32),
                pltpu.VMEM((group // 2, 2 * bag), jnp.int32),
                pltpu.VMEM((group * (blocks + 8), BLK), F32),
            ],
        ),
        out_shape=jax.ShapeDtypeStruct((blocks, share, BLK), BF16),
        name="count_bags",
    )(rank, index, length)


def pool_kernel(
    held_ref, wanted_ref, counts_ref, part0, part1, part2, part3, pooled_ref, moved_ref,
    split_rows, total, target,
):
    step = pl.program_id(0)
    parts = (part0, part1, part2, part3)
    slots = part0.shape[0]
    width = part0.shape[2]

    @pl.when(step == 0)
    def _():
        for b in range(len(parts) * slots):
            target[b] = -1
        for s in range(slots):
            target[wanted_ref[s]] = s
        for k, part in enumerate(parts):
            for s in range(slots):
                b = held_ref[k * slots + s]
                rows = part[s]
                top, rest = halves(rows)
                split_rows[b, :, :width] = top
                split_rows[b, :, width:] = rest
                goal = target[b]

                @pl.when(goal >= 0)
                def _(part=part, s=s, goal=goal):
                    moved_ref[goal] = part[s]

    pair = counts_ref.shape[0]
    left = jnp.concatenate([counts_ref[k] for k in range(pair)], axis=1)
    right = split_rows[pl.ds(step * pair, pair)].reshape(pair * BLK, 2 * width)
    found = lax.dot_general(left, right, (((1,), (0,)), ((), ())), preferred_element_type=F32)

    @pl.when(step == 0)
    def _():
        total[...] = found

    @pl.when(step > 0)
    def _():
        total[...] += found

    @pl.when(step == pl.num_programs(0) - 1)
    def _():
        pooled_ref[...] = total[:, :width] + total[:, width:]


def pool_and_move(held, wanted, counts, parts):
    blocks, share, _ = counts.shape
    slots, _, width = parts[0].shape
    pair = 2
    whole = pl.BlockSpec((slots, BLK, width), lambda j, *_: (0, 0, 0))
    return pl.pallas_call(
        pool_kernel,
        grid_spec=pltpu.PrefetchScalarGridSpec(
            num_scalar_prefetch=2,
            grid=(blocks // pair,),
            in_specs=[pl.BlockSpec((pair, share, BLK), lambda j, *_: (j, 0, 0))] + [whole] * 4,
            out_specs=[
                pl.BlockSpec((share, width), lambda j, *_: (0, 0)),
                whole,
            ],
            scratch_shapes=[
                pltpu.VMEM((blocks, BLK, 2 * width), BF16),
                pltpu.VMEM((share, 2 * width), F32),
                pltpu.SMEM((blocks,), jnp.int32),
            ],
        ),
        out_shape=[
            jax.ShapeDtypeStruct((share, width), F32),
            jax.ShapeDtypeStruct((slots, BLK, width), F32),
        ],
        name="pool_and_move",
    )(held, wanted, counts, *parts)


def top_kernel(
    pooled_ref, dense_ref, first_hbm, second_hbm, out_ref, logits_ref,
    first, second, gram, joined, sems,
):
    samples, width = dense_ref.shape
    tables = pooled_ref.shape[0] // samples
    pitch = gram.shape[0] // samples
    inputs = first_hbm.shape[0]
    fetch_first = pltpu.make_async_copy(first_hbm, first.at[pl.ds(0, inputs)], sems.at[0])
    fetch_second = pltpu.make_async_copy(second_hbm, second, sems.at[1])
    fetch_first.start()
    fetch_second.start()
    first[inputs:, :] = jnp.zeros((first.shape[0] - inputs, first.shape[1]), BF16)
    dense = dense_ref[...].astype(F32)
    for s in range(samples):
        top, rest = halves(pooled_ref[pl.ds(s, tables, stride=samples), :])
        own = jnp.broadcast_to(dense[s : s + 1], (8, width)).astype(BF16)
        none = jnp.zeros((8, width), BF16)
        tall_top = jnp.concatenate([top, own], axis=0)
        tall_rest = jnp.concatenate([rest, none], axis=0)
        left = jnp.concatenate([tall_top, tall_rest, tall_top], axis=1)
        right = jnp.concatenate([top, top, rest], axis=1)
        found = lax.dot_general(
            left, right, (((1,), (1,)), ((), ())), preferred_element_type=F32
        )
        gram[s * pitch : (s + 1) * pitch, :tables] = found * width ** (-0.5)
    lane = lax.broadcasted_iota(jnp.int32, (samples, 128), 1)
    joined[:, :width] = dense_ref[...]
    at = width
    filling = jnp.zeros((samples, 128), F32)
    for i in range(-1, tables - 1):
        row = tables if i < 0 else i
        start = 0 if i < 0 else i + 1
        line = gram[pl.ds(row, samples, stride=pitch), :]
        shift = (at - start) % 128
        line = pltpu.roll(line, shift, 1) if shift else line
        filling = jnp.where(lane >= at % 128, line, filling)
        after = at + tables - start
        if after // 128 != at // 128:
            base = at // 128 * 128
            joined[:, base : base + 128] = filling.astype(BF16)
            filling = line
        at = after
    base = at // 128 * 128
    if at % 128:
        joined[:, base : base + 128] = jnp.where(lane < at % 128, filling, 0.0).astype(BF16)
    fetch_first.wait()
    hidden = jnp.dot(joined[...], first[...], preferred_element_type=F32)
    hidden = jnp.maximum(hidden, 0.0).astype(BF16)
    fetch_second.wait()
    hidden = jnp.dot(hidden, second[...], preferred_element_type=F32)
    hidden = jnp.maximum(hidden, 0.0).astype(BF16)
    last = jnp.broadcast_to(out_ref[...], (16, hidden.shape[1]))
    answer = lax.dot_general(last, hidden, (((1,), (1,)), ((), ())), preferred_element_type=F32)
    logits_ref[...] = answer[:1]


def top_of_model(pooled, dense, w_first, w_second, w_out):
    samples, width = dense.shape
    tables = pooled.shape[0] // samples
    inputs, hidden = w_first.shape
    padded = -(-inputs // 128) * 128
    vmem = pl.BlockSpec(memory_space=pltpu.VMEM)
    hbm = pl.BlockSpec(memory_space=pl.ANY)
    return pl.pallas_call(
        top_kernel,
        in_specs=[vmem, vmem, hbm, hbm, vmem],
        out_specs=vmem,
        out_shape=jax.ShapeDtypeStruct((1, samples), F32),
        scratch_shapes=[
            pltpu.VMEM((padded, hidden), BF16),
            pltpu.VMEM(w_second.shape, BF16),
            pltpu.VMEM((samples * (tables + 8), 128), F32),
            pltpu.VMEM((samples, padded), BF16),
            pltpu.SemaphoreType.DMA((2,)),
        ],
        name="top_of_model",
    )(pooled, dense, w_first, w_second, w_out.reshape(1, -1))


def shards(
    old_table, old_blocks, new_blocks, bag_row_index, bag_length, dense, w_first, w_second, w_out
):
    slots = old_blocks.shape[1]
    width = old_table.shape[2]
    rows = lax.axis_size("row")
    rank = lax.axis_index("row")
    own = old_table[0].reshape(slots, BLK, width)
    other_core = [(k, k ^ 1) for k in range(rows)]
    other_chip = [(k, k ^ 2) for k in range(rows)]
    both = [(k, k ^ 3) for k in range(rows)]
    ids = old_blocks[0]
    across = lax.ppermute(own, "row", other_chip)
    beside = lax.ppermute(own, "row", other_core)
    far = lax.ppermute(across, "row", other_core)
    held = jnp.concatenate(
        [
            ids,
            lax.ppermute(ids, "row", other_core),
            lax.ppermute(ids, "row", other_chip),
            lax.ppermute(ids, "row", both),
        ]
    )
    share = bag_row_index.shape[0] // rows
    counts = count_bags(
        rank.astype(jnp.int32)[None],
        jnp.transpose(bag_row_index[:, 0, :]),
        jnp.transpose(bag_length),
        share,
        rows * slots,
    )
    pooled, moved = pool_and_move(held, new_blocks[0], counts, (own, beside, across, far))
    cols = lax.axis_size("col")
    spread = lax.all_to_all(
        pooled.reshape(cols, share // cols, width), "col", split_axis=0, concat_axis=0, tiled=True
    )
    logits = top_of_model(spread.reshape(share, width), dense, w_first, w_second, w_out)
    return logits.reshape(-1), moved.reshape(1, slots * BLK, width)


def solution(mesh):
    in_specs = (
        P("col", "row", None),
        P("col", "row"),
        P("col", "row"),
        P(None, "col", None),
        P(None, "col"),
        P(("row", "col"), None),
        P(),
        P(),
        P(),
    )
    out_specs = (P(("row", "col")), P("col", "row", None))
    return jax.shard_map(shards, mesh=mesh, in_specs=in_specs, out_specs=out_specs, check_vma=False)
```

```python
import functools

import jax
import jax.numpy as jnp
from jax import lax
from jax.experimental import pallas as pl
from jax.experimental.pallas import tpu as pltpu
from jax.sharding import PartitionSpec as P


BLK = 128
BF16 = jnp.bfloat16
F32 = jnp.float32


def halves(x):
    top = x.astype(BF16)
    rest = (x - top.astype(F32)).astype(BF16)
    return top, rest


def in_vmem(x):
    return pltpu.with_memory_space_constraint(x, pltpu.VMEM)


def in_hbm(x):
    return pltpu.with_memory_space_constraint(x, pltpu.HBM)


def count_kernel(rank_ref, index_hbm, length_hbm, counts_ref, index, length, staged, sems):
    bag, share = index.shape
    blocks = counts_ref.shape[0]
    group = 128
    pitch = staged.shape[0] // group
    start = pl.multiple_of(rank_ref[0] * share, 128)
    fetch_index = pltpu.make_async_copy(index_hbm.at[:, pl.ds(start, share)], index, sems.at[0])
    fetch_length = pltpu.make_async_copy(length_hbm.at[:, pl.ds(start, share)], length, sems.at[1])
    fetch_index.start()
    fetch_length.start()
    fetch_index.wait()
    fetch_length.wait()
    place = lax.broadcasted_iota(jnp.int32, (bag, group), 0)
    offset_order = lax.broadcasted_iota(jnp.int32, (2 * bag, BLK), 1).astype(F32).astype(BF16)
    block_order = lax.broadcasted_iota(jnp.int32, (2 * blocks, 2 * bag), 0)
    one = jnp.ones((), BF16)
    none = jnp.zeros((), BF16)

    def some(step, carry):
        base = pl.multiple_of(step * group, group)
        rows = index[:, pl.ds(base, group)]
        rows = jnp.where(place < length[:, pl.ds(base, group)], rows, -1)
        offset = (rows & (BLK - 1)).astype(F32).astype(BF16)
        rows = jnp.transpose(rows, (1, 0))
        block = jnp.where(rows < 0, -1, lax.shift_right_arithmetic(rows, 7))
        second = jnp.where(block < 0, -1, block + blocks)
        for first in range(0, group, 16):
            key = jnp.concatenate([block[first : first + 8], second[first + 8 : first + 16]], axis=1)
            for k in range(8):
                n = first + k
                column = jnp.concatenate([offset[:, n : n + 1], offset[:, n + 8 : n + 9]], axis=0)
                in_block = jnp.where(key[k : k + 1] == block_order, 1.0, 0.0).astype(BF16)
                at_offset = jnp.where(column == offset_order, one, none)
                found = jnp.dot(in_block, at_offset, preferred_element_type=F32)
                staged[n * pitch : n * pitch + blocks, :] = found[:blocks]
                staged[(n + 8) * pitch : (n + 8) * pitch + blocks, :] = found[blocks:]
            for b in range(blocks):
                sixteen = staged[pl.ds(first * pitch + b, 16, stride=pitch), :].astype(BF16)
                counts_ref[b, pl.ds(pl.multiple_of(base + first, 16), 16), :] = sixteen
        return carry

    lax.fori_loop(0, share // group, some, 0)


def count_bags(rank, index, length, share, blocks):
    bag = index.shape[0]
    hbm = pl.BlockSpec(memory_space=pltpu.HBM)
    return pl.pallas_call(
        count_kernel,
        in_specs=[pl.BlockSpec(memory_space=pltpu.SMEM), hbm, hbm],
        out_specs=pl.BlockSpec(memory_space=pltpu.VMEM),
        out_shape=pltpu.VMEM((blocks, share, BLK), BF16),
        scratch_shapes=[
            pltpu.VMEM((bag, share), jnp.int32),
            pltpu.VMEM((1, share), jnp.int32),
            pltpu.VMEM((128 * (blocks + 4), BLK), F32),
            pltpu.SemaphoreType.DMA((2,)),
        ],
        cost_estimate=pl.CostEstimate(
            flops=40 << 30, bytes_accessed=8388608, transcendentals=0
        ),
        compiler_params=pltpu.CompilerParams(vmem_limit_bytes=16 << 20),
        name="count_bags",
    )(rank, in_hbm(index), in_hbm(length))


def pool_kernel(first_slot, has_prior, held_ref, counts_ref, *refs):
    refs = list(refs)
    split_rows = refs.pop()
    pooled_ref = refs.pop()
    prior_ref = refs.pop() if has_prior else None
    slots, _, width = refs[0].shape
    for k, part in enumerate(refs):
        for s in range(slots):
            at = (k * slots + s) * BLK
            top, rest = halves(part[s])
            split_rows[at : at + BLK, :width] = top
            split_rows[at : at + BLK, width:] = rest
    total = len(refs) * slots
    left = jnp.concatenate([counts_ref[held_ref[first_slot + q]] for q in range(total)], axis=1)
    found = jnp.dot(left, split_rows[...], preferred_element_type=F32)
    found = found[:, :width] + found[:, width:]
    pooled_ref[...] = found + prior_ref[...] if has_prior else found


def pool(held, first_slot, counts, parts, prior, keep):
    _, share, _ = counts.shape
    slots, _, width = parts[0].shape
    vmem = pl.BlockSpec(memory_space=pltpu.VMEM)
    arrays = [counts, *parts] + ([] if prior is None else [prior])
    return pl.pallas_call(
        functools.partial(pool_kernel, first_slot, prior is not None),
        in_specs=[pl.BlockSpec(memory_space=pltpu.SMEM)] + [vmem] * len(arrays),
        out_specs=vmem,
        out_shape=pltpu.VMEM((share, width), F32) if keep else pltpu.HBM((share, width), F32),
        scratch_shapes=[pltpu.VMEM((len(parts) * slots * BLK, 2 * width), BF16)],
        cost_estimate=pl.CostEstimate(
            flops=2 * share * len(parts) * slots * BLK * 2 * width,
            bytes_accessed=4 << 20,
            transcendentals=0,
        ),
        compiler_params=pltpu.CompilerParams(vmem_limit_bytes=24 << 20),
        name="pool",
    )(held, *[in_vmem(a) for a in arrays])


def move_kernel(held_ref, wanted_ref, part0, part1, part2, part3, moved_ref, target, sem):
    parts = (part0, part1, part2, part3)
    slots = part0.shape[0]
    for b in range(len(parts) * slots):
        target[b] = -1
    for s in range(slots):
        target[wanted_ref[s]] = s
    for k, part in enumerate(parts):
        for s in range(slots):
            goal = target[held_ref[k * slots + s]]

            @pl.when(goal >= 0)
            def _(part=part, s=s, goal=goal):
                pltpu.make_async_copy(part.at[s], moved_ref.at[goal], sem).start()

    pltpu.make_async_copy(part0, moved_ref, sem).wait()


def move_blocks(held, wanted, parts):
    slots, _, width = parts[0].shape
    smem = pl.BlockSpec(memory_space=pltpu.SMEM)
    hbm = pl.BlockSpec(memory_space=pltpu.HBM)
    return pl.pallas_call(
        move_kernel,
        in_specs=[smem, smem] + [pl.BlockSpec(memory_space=pltpu.VMEM)] * 4,
        out_specs=hbm,
        out_shape=jax.ShapeDtypeStruct((slots, BLK, width), F32),
        scratch_shapes=[pltpu.SMEM((len(parts) * slots,), jnp.int32), pltpu.SemaphoreType.DMA],
        compiler_params=pltpu.CompilerParams(vmem_limit_bytes=4 << 20),
        name="move_blocks",
    )(held, wanted, *[in_vmem(part) for part in parts])


def top_kernel(
    pooled_ref, dense_ref, first_hbm, second_hbm, out_ref, logits_ref,
    first_ref, second_ref, gram, joined, sems,
):
    samples, width = dense_ref.shape
    tables = pooled_ref.shape[0] // samples
    pitch = gram.shape[0] // samples
    inputs = first_ref.shape[0]
    fetch_first = pltpu.make_async_copy(first_hbm, first_ref, sems.at[0])
    fetch_second = pltpu.make_async_copy(second_hbm, second_ref, sems.at[1])
    fetch_first.start()
    fetch_second.start()
    whole = inputs // 128 * 128
    dense = dense_ref[...].astype(F32)
    for s in range(samples):
        top, rest = halves(pooled_ref[pl.ds(s, tables, stride=samples), :])
        own = jnp.broadcast_to(dense[s : s + 1], (8, width)).astype(BF16)
        none = jnp.zeros((8, width), BF16)
        tall_top = jnp.concatenate([top, own], axis=0)
        tall_rest = jnp.concatenate([rest, none], axis=0)
        left = jnp.concatenate([tall_top, tall_rest, tall_top], axis=1)
        right = jnp.concatenate([top, top, rest], axis=1)
        found = lax.dot_general(
            left, right, (((1,), (1,)), ((), ())), preferred_element_type=F32
        )
        gram[s * pitch : (s + 1) * pitch, :tables] = found * width ** (-0.5)
    lane = lax.broadcasted_iota(jnp.int32, (samples, 128), 1)
    joined[:, :width] = dense_ref[...]
    at = width
    filling = jnp.zeros((samples, 128), F32)
    for i in range(-1, tables - 1):
        row = tables if i < 0 else i
        start = 0 if i < 0 else i + 1
        line = gram[pl.ds(row, samples, stride=pitch), :]
        shift = (at - start) % 128
        line = pltpu.roll(line, shift, 1) if shift else line
        filling = jnp.where(lane >= at % 128, line, filling)
        after = at + tables - start
        if after // 128 != at // 128:
            base = at // 128 * 128
            joined[:, base : base + 128] = filling.astype(BF16)
            filling = line
        at = after
    base = at // 128 * 128
    if at % 128:
        joined[:, base : base + 128] = jnp.where(lane < at % 128, filling, 0.0).astype(BF16)
    fetch_first.wait()
    hidden = jnp.dot(joined[:, :whole], first_ref[:whole], preferred_element_type=F32)
    if inputs > whole:
        last = jnp.dot(joined[:, whole:inputs], first_ref[whole:], preferred_element_type=F32)
        hidden = hidden + last
    hidden = jnp.maximum(hidden, 0.0).astype(BF16)
    fetch_second.wait()
    hidden = jnp.dot(hidden, second_ref[...], preferred_element_type=F32)
    hidden = jnp.maximum(hidden, 0.0).astype(BF16)
    last = jnp.broadcast_to(out_ref[...], (16, hidden.shape[1]))
    answer = lax.dot_general(last, hidden, (((1,), (1,)), ((), ())), preferred_element_type=F32)
    logits_ref[...] = answer[:1]


def top_of_model(pooled, dense, w_first, w_second, w_out):
    samples, _ = dense.shape
    tables = pooled.shape[0] // samples
    inputs, _ = w_first.shape
    padded = -(-inputs // 128) * 128
    hbm = pl.BlockSpec(memory_space=pltpu.HBM)
    vmem = pl.BlockSpec(memory_space=pltpu.VMEM)
    return pl.pallas_call(
        top_kernel,
        in_specs=[vmem, vmem, hbm, hbm, vmem],
        out_specs=vmem,
        out_shape=jax.ShapeDtypeStruct((1, samples), F32),
        scratch_shapes=[
            pltpu.VMEM(w_first.shape, BF16),
            pltpu.VMEM(w_second.shape, BF16),
            pltpu.VMEM((samples * (tables + 8), 128), F32),
            pltpu.VMEM((samples, padded), BF16),
            pltpu.SemaphoreType.DMA((2,)),
        ],
        compiler_params=pltpu.CompilerParams(vmem_limit_bytes=16 << 20),
        name="top_of_model",
    )(in_vmem(pooled), dense, in_hbm(w_first), in_hbm(w_second), w_out.reshape(1, -1))


def shards(
    old_table, old_blocks, new_blocks, bag_row_index, bag_length, dense, w_first, w_second, w_out
):
    slots = old_blocks.shape[1]
    width = old_table.shape[2]
    rows = lax.axis_size("row")
    rank = lax.axis_index("row")
    own = old_table[0].reshape(slots, BLK, width)
    other_core = [(k, k ^ 1) for k in range(rows)]
    other_chip = [(k, k ^ 2) for k in range(rows)]
    both = [(k, k ^ 3) for k in range(rows)]
    ids = old_blocks[0]
    across = lax.ppermute(own, "row", other_chip)
    beside = lax.ppermute(own, "row", other_core)
    named = [ids]
    for pairs in (other_core, other_chip, both):
        named.append(lax.ppermute(ids, "row", pairs))
    held = jnp.concatenate(named)
    share = bag_row_index.shape[0] // rows
    counts = count_bags(
        rank.astype(jnp.int32)[None],
        jnp.transpose(bag_row_index[:, 0, :]),
        jnp.transpose(bag_length),
        share,
        rows * slots,
    )
    far = lax.ppermute(across, "row", other_core)
    pooled = pool(held, 0, counts, (own, beside, across), None, True)
    pooled = pool(held, 3 * slots, counts, (far,), pooled, False)
    moved = move_blocks(held, new_blocks[0], (own, beside, across, far))
    cols = lax.axis_size("col")
    pooled = pooled.reshape(cols, share // cols, width)
    spread = lax.all_to_all(pooled, "col", split_axis=0, concat_axis=0, tiled=True)
    logits = top_of_model(spread.reshape(share, width), dense, w_first, w_second, w_out)
    return logits.reshape(-1), moved.reshape(1, slots * BLK, width)


def solution(mesh):
    in_specs = (
        P("col", "row", None),
        P("col", "row"),
        P("col", "row"),
        P(None, "col", None),
        P(None, "col"),
        P(("row", "col"), None),
        P(),
        P(),
        P(),
    )
    out_specs = (P(("row", "col")), P("col", "row", None))

    return jax.shard_map(shards, mesh=mesh, in_specs=in_specs, out_specs=out_specs, check_vma=False)
```

```python
import functools

import jax
import jax.numpy as jnp
from jax import lax
from jax.experimental import pallas as pl
from jax.experimental.pallas import tpu as pltpu
from jax.sharding import PartitionSpec as P


BLK = 128
FETCH = 256
BF16 = jnp.bfloat16
F32 = jnp.float32


def halves(x):
    top = x.astype(BF16)
    rest = (x - top.astype(F32)).astype(BF16)
    return top, rest


def in_vmem(x):
    return pltpu.with_memory_space_constraint(x, pltpu.VMEM)


def in_hbm(x):
    return pltpu.with_memory_space_constraint(x, pltpu.HBM)


def count_kernel(rank_ref, index_hbm, length_hbm, counts_ref, index, length, staged, sems):
    bag, share = index.shape
    blocks = counts_ref.shape[0]
    group = 256
    pitch = staged.shape[0] // group
    start = pl.multiple_of(rank_ref[0] * share, 128)
    fetch_index = pltpu.make_async_copy(index_hbm.at[:, pl.ds(start, share)], index, sems.at[0])
    fetch_length = pltpu.make_async_copy(length_hbm.at[:, pl.ds(start, share)], length, sems.at[1])
    fetch_index.start()
    fetch_length.start()
    fetch_index.wait()
    fetch_length.wait()
    place = lax.broadcasted_iota(jnp.int32, (bag, group), 0)
    offset_order = lax.broadcasted_iota(jnp.int32, (2 * bag, BLK), 1).astype(F32).astype(BF16)
    block_order = lax.broadcasted_iota(jnp.int32, (2 * blocks, 2 * bag), 0)
    one = jnp.ones((), BF16)
    none = jnp.zeros((), BF16)

    def some(step, carry):
        base = pl.multiple_of(step * group, group)
        rows = index[:, pl.ds(base, group)]
        rows = jnp.where(place < length[:, pl.ds(base, group)], rows, -1)
        offset = (rows & (BLK - 1)).astype(F32).astype(BF16)
        rows = jnp.transpose(rows, (1, 0))
        block = jnp.where(rows < 0, -1, lax.shift_right_arithmetic(rows, 7))
        second = jnp.where(block < 0, -1, block + blocks)
        for first in range(0, group, 16):
            key = jnp.concatenate([block[first : first + 8], second[first + 8 : first + 16]], axis=1)
            for k in range(8):
                n = first + k
                column = jnp.concatenate([offset[:, n : n + 1], offset[:, n + 8 : n + 9]], axis=0)
                in_block = jnp.where(key[k : k + 1] == block_order, 1.0, 0.0).astype(BF16)
                at_offset = jnp.where(column == offset_order, one, none)
                found = jnp.dot(in_block, at_offset, preferred_element_type=F32)
                staged[n * pitch : n * pitch + blocks, :] = found[:blocks]
                staged[(n + 8) * pitch : (n + 8) * pitch + blocks, :] = found[blocks:]
            for b in range(blocks):
                sixteen = staged[pl.ds(first * pitch + b, 16, stride=pitch), :].astype(BF16)
                counts_ref[b, pl.ds(pl.multiple_of(base + first, 16), 16), :] = sixteen
        return carry

    lax.fori_loop(0, share // group, some, 0)


def count_bags(rank, index, length, share, blocks):
    bag = index.shape[0]
    hbm = pl.BlockSpec(memory_space=pltpu.HBM)
    return pl.pallas_call(
        count_kernel,
        in_specs=[pl.BlockSpec(memory_space=pltpu.SMEM), hbm, hbm],
        out_specs=pl.BlockSpec(memory_space=pltpu.VMEM),
        out_shape=pltpu.VMEM((blocks, share, BLK), BF16),
        scratch_shapes=[
            pltpu.VMEM((bag, share), jnp.int32),
            pltpu.VMEM((1, share), jnp.int32),
            pltpu.VMEM((256 * (blocks + 4), BLK), F32),
            pltpu.SemaphoreType.DMA((2,)),
        ],
        cost_estimate=pl.CostEstimate(
            flops=40 << 30, bytes_accessed=8388608, transcendentals=0
        ),
        compiler_params=pltpu.CompilerParams(vmem_limit_bytes=16 << 20),
        name="count_bags",
    )(rank, in_hbm(index), in_hbm(length))


def pool_kernel(first_slot, has_prior, held_ref, counts_ref, *refs):
    refs = list(refs)
    split_rows = refs.pop()
    pooled_ref = refs.pop()
    prior_ref = refs.pop() if has_prior else None
    slots, _, width = refs[0].shape
    for k, part in enumerate(refs):
        for s in range(slots):
            at = (k * slots + s) * BLK
            top, rest = halves(part[s])
            split_rows[at : at + BLK, :width] = top
            split_rows[at : at + BLK, width:] = rest
    total = len(refs) * slots
    left = jnp.concatenate([counts_ref[held_ref[first_slot + q]] for q in range(total)], axis=1)
    found = jnp.dot(left, split_rows[...], preferred_element_type=F32)
    found = found[:, :width] + found[:, width:]
    pooled_ref[...] = found + prior_ref[...] if has_prior else found


def pool(held, first_slot, counts, parts, prior, keep):
    _, share, _ = counts.shape
    slots, _, width = parts[0].shape
    vmem = pl.BlockSpec(memory_space=pltpu.VMEM)
    arrays = [counts, *parts] + ([] if prior is None else [prior])
    return pl.pallas_call(
        functools.partial(pool_kernel, first_slot, prior is not None),
        in_specs=[pl.BlockSpec(memory_space=pltpu.SMEM)] + [vmem] * len(arrays),
        out_specs=vmem,
        out_shape=pltpu.VMEM((share, width), F32) if keep else pltpu.HBM((share, width), F32),
        scratch_shapes=[pltpu.VMEM((len(parts) * slots * BLK, 2 * width), BF16)],
        cost_estimate=pl.CostEstimate(
            flops=2 * share * len(parts) * slots * BLK * 2 * width,
            bytes_accessed=4 << 20,
            transcendentals=0,
        ),
        compiler_params=pltpu.CompilerParams(vmem_limit_bytes=24 << 20),
        name="pool",
    )(held, *[in_vmem(a) for a in arrays])


def move_kernel(held_ref, wanted_ref, part0, part1, part2, part3, moved_ref, target, sem):
    parts = (part0, part1, part2, part3)
    slots = part0.shape[0]
    for b in range(len(parts) * slots):
        target[b] = -1
    for s in range(slots):
        target[wanted_ref[s]] = s
    for k, part in enumerate(parts):
        for s in range(slots):
            goal = target[held_ref[k * slots + s]]

            @pl.when(goal >= 0)
            def _(part=part, s=s, goal=goal):
                pltpu.make_async_copy(part.at[s], moved_ref.at[goal], sem).start()

    pltpu.make_async_copy(part0, moved_ref, sem).wait()


def move_blocks(held, wanted, parts):
    slots, _, width = parts[0].shape
    smem = pl.BlockSpec(memory_space=pltpu.SMEM)
    hbm = pl.BlockSpec(memory_space=pltpu.HBM)
    return pl.pallas_call(
        move_kernel,
        in_specs=[smem, smem] + [pl.BlockSpec(memory_space=pltpu.VMEM)] * 4,
        out_specs=hbm,
        out_shape=jax.ShapeDtypeStruct((slots, BLK, width), F32),
        scratch_shapes=[pltpu.SMEM((len(parts) * slots,), jnp.int32), pltpu.SemaphoreType.DMA],
        compiler_params=pltpu.CompilerParams(vmem_limit_bytes=4 << 20),
        name="move_blocks",
    )(held, wanted, *[in_vmem(part) for part in parts])


def top_kernel(
    pooled_ref, dense_ref, first_hbm, second_hbm, out_ref, logits_ref,
    first_ref, second_ref, gram, joined, sems,
):
    samples, width = dense_ref.shape
    tables = pooled_ref.shape[0] // samples
    pitch = gram.shape[0] // samples
    inputs = first_ref.shape[0]
    depth = second_ref.shape[0]
    pieces = [(first_hbm, first_ref, at, min(FETCH, inputs - at)) for at in range(0, inputs, FETCH)]
    layer = len(pieces)
    pieces += [(second_hbm, second_ref, at, min(FETCH, depth - at)) for at in range(0, depth, FETCH)]
    fetches = [
        pltpu.make_async_copy(there.at[pl.ds(at, size)], here.at[pl.ds(at, size)], sems.at[k])
        for k, (there, here, at, size) in enumerate(pieces)
    ]
    for fetch in fetches:
        fetch.start()
    dense = dense_ref[...].astype(F32)
    for s in range(samples):
        top, rest = halves(pooled_ref[pl.ds(s, tables, stride=samples), :])
        own = jnp.broadcast_to(dense[s : s + 1], (8, width)).astype(BF16)
        none = jnp.zeros((8, width), BF16)
        tall_top = jnp.concatenate([top, own], axis=0)
        tall_rest = jnp.concatenate([rest, none], axis=0)
        left = jnp.concatenate([tall_top, tall_rest, tall_top], axis=1)
        right = jnp.concatenate([top, top, rest], axis=1)
        found = lax.dot_general(
            left, right, (((1,), (1,)), ((), ())), preferred_element_type=F32
        )
        gram[s * pitch : (s + 1) * pitch, :tables] = found * width ** (-0.5)
    lane = lax.broadcasted_iota(jnp.int32, (samples, 128), 1)
    joined[:, :width] = dense_ref[...]
    at = width
    filling = jnp.zeros((samples, 128), F32)
    for i in range(-1, tables - 1):
        row = tables if i < 0 else i
        start = 0 if i < 0 else i + 1
        line = gram[pl.ds(row, samples, stride=pitch), :]
        shift = (at - start) % 128
        line = pltpu.roll(line, shift, 1) if shift else line
        filling = jnp.where(lane >= at % 128, line, filling)
        after = at + tables - start
        if after // 128 != at // 128:
            base = at // 128 * 128
            joined[:, base : base + 128] = filling.astype(BF16)
            filling = line
        at = after
    base = at // 128 * 128
    if at % 128:
        joined[:, base : base + 128] = jnp.where(lane < at % 128, filling, 0.0).astype(BF16)
    hidden = jnp.zeros((samples, first_ref.shape[1]), F32)
    for fetch, (_, _, at, size) in zip(fetches[:layer], pieces[:layer]):
        fetch.wait()
        whole = size // 128 * 128
        for begin, count in ((at, whole), (at + whole, size - whole)):
            if count:
                ends = slice(begin, begin + count)
                hidden += jnp.dot(joined[:, ends], first_ref[ends], preferred_element_type=F32)
    value = jnp.maximum(hidden, 0.0).astype(BF16)
    hidden = jnp.zeros((samples, second_ref.shape[1]), F32)
    for fetch, (_, _, at, size) in zip(fetches[layer:], pieces[layer:]):
        fetch.wait()
        ends = slice(at, at + size)
        hidden += jnp.dot(value[:, ends], second_ref[ends], preferred_element_type=F32)
    hidden = jnp.maximum(hidden, 0.0).astype(BF16)
    last = jnp.broadcast_to(out_ref[...], (16, hidden.shape[1]))
    answer = lax.dot_general(last, hidden, (((1,), (1,)), ((), ())), preferred_element_type=F32)
    logits_ref[...] = answer[:1]


def top_of_model(pooled, dense, w_first, w_second, w_out):
    samples, _ = dense.shape
    tables = pooled.shape[0] // samples
    inputs, _ = w_first.shape
    padded = -(-inputs // 128) * 128
    hbm = pl.BlockSpec(memory_space=pltpu.HBM)
    vmem = pl.BlockSpec(memory_space=pltpu.VMEM)
    return pl.pallas_call(
        top_kernel,
        in_specs=[vmem, vmem, hbm, hbm, vmem],
        out_specs=vmem,
        out_shape=jax.ShapeDtypeStruct((1, samples), F32),
        scratch_shapes=[
            pltpu.VMEM(w_first.shape, BF16),
            pltpu.VMEM(w_second.shape, BF16),
            pltpu.VMEM((samples * (tables + 8), 128), F32),
            pltpu.VMEM((samples, padded), BF16),
            pltpu.SemaphoreType.DMA((-(-inputs // FETCH) - (-w_second.shape[0] // FETCH),)),
        ],
        compiler_params=pltpu.CompilerParams(vmem_limit_bytes=16 << 20),
        name="top_of_model",
    )(in_vmem(pooled), dense, in_hbm(w_first), in_hbm(w_second), w_out.reshape(1, -1))


def shards(
    old_table, old_blocks, new_blocks, bag_row_index, bag_length, dense, w_first, w_second, w_out
):
    slots = old_blocks.shape[1]
    width = old_table.shape[2]
    rows = lax.axis_size("row")
    rank = lax.axis_index("row")
    own = old_table[0].reshape(slots, BLK, width)
    other_core = [(k, k ^ 1) for k in range(rows)]
    other_chip = [(k, k ^ 2) for k in range(rows)]
    both = [(k, k ^ 3) for k in range(rows)]
    ids = old_blocks[0]
    across = lax.ppermute(own, "row", other_chip)
    beside = lax.ppermute(own, "row", other_core)
    named = [ids]
    for pairs in (other_core, other_chip, both):
        named.append(lax.ppermute(ids, "row", pairs))
    held = jnp.concatenate(named)
    share = bag_row_index.shape[0] // rows
    counts = count_bags(
        rank.astype(jnp.int32)[None],
        jnp.transpose(bag_row_index[:, 0, :]),
        jnp.transpose(bag_length),
        share,
        rows * slots,
    )
    far = lax.ppermute(across, "row", other_core)
    pooled = pool(held, 0, counts, (own, beside, across), None, True)
    pooled = pool(held, 3 * slots, counts, (far,), pooled, False)
    moved = move_blocks(held, new_blocks[0], (own, beside, across, far))
    cols = lax.axis_size("col")
    pooled = pooled.reshape(cols, share // cols, width)
    spread = lax.all_to_all(pooled, "col", split_axis=0, concat_axis=0, tiled=True)
    logits = top_of_model(spread.reshape(share, width), dense, w_first, w_second, w_out)
    return logits.reshape(-1), moved.reshape(1, slots * BLK, width)


def solution(mesh):
    in_specs = (
        P("col", "row", None),
        P("col", "row"),
        P("col", "row"),
        P(None, "col", None),
        P(None, "col"),
        P(("row", "col"), None),
        P(),
        P(),
        P(),
    )
    out_specs = (P(("row", "col")), P("col", "row", None))

    return jax.shard_map(shards, mesh=mesh, in_specs=in_specs, out_specs=out_specs, check_vma=False)
```

```python
import functools

import jax
import jax.numpy as jnp
from jax import lax
from jax.experimental import pallas as pl
from jax.experimental.pallas import tpu as pltpu
from jax.sharding import PartitionSpec as P


BLK = 128
FETCH = 256
BF16 = jnp.bfloat16
F32 = jnp.float32


def halves(x):
    top = x.astype(BF16)
    rest = (x - top.astype(F32)).astype(BF16)
    return top, rest


def in_vmem(x):
    return pltpu.with_memory_space_constraint(x, pltpu.VMEM)


def in_hbm(x):
    return pltpu.with_memory_space_constraint(x, pltpu.HBM)


def pooled_part(ids, counts_ref, parts, split_rows):
    slots, _, width = parts[0].shape
    for k, part in enumerate(parts):
        for s in range(slots):
            at = (k * slots + s) * BLK
            top, rest = halves(part[s])
            split_rows[at : at + BLK, :width] = top
            split_rows[at : at + BLK, width:] = rest
    left = jnp.concatenate([counts_ref[b] for b in ids], axis=1)
    found = jnp.dot(left, split_rows[...], preferred_element_type=F32)
    return found[:, :width] + found[:, width:]


def count_kernel(
    rank_ref, ids_hbm, index_hbm, length_hbm, own_hbm, counts_ref, pooled_ref,
    ids, index, length, staged, own, split_rows, sems,
):
    bag, share = index.shape
    blocks = counts_ref.shape[0]
    group = 256
    pitch = staged.shape[0] // group
    start = pl.multiple_of(rank_ref[0] * share, 128)
    fetch_index = pltpu.make_async_copy(index_hbm.at[:, pl.ds(start, share)], index, sems.at[0])
    fetch_length = pltpu.make_async_copy(length_hbm.at[:, pl.ds(start, share)], length, sems.at[1])
    fetch_ids = pltpu.make_async_copy(ids_hbm, ids, sems.at[3])
    fetch_own = pltpu.make_async_copy(own_hbm, own, sems.at[2])
    fetch_index.start()
    fetch_length.start()
    fetch_own.start()
    fetch_ids.start()
    fetch_index.wait()
    fetch_length.wait()
    place = lax.broadcasted_iota(jnp.int32, (bag, group), 0)
    offset_order = lax.broadcasted_iota(jnp.int32, (2 * bag, BLK), 1).astype(F32).astype(BF16)
    block_order = lax.broadcasted_iota(jnp.int32, (2 * blocks, 2 * bag), 0)
    one = jnp.ones((), BF16)
    none = jnp.zeros((), BF16)

    def some(step, carry):
        base = pl.multiple_of(step * group, group)
        rows = index[:, pl.ds(base, group)]
        rows = jnp.where(place < length[:, pl.ds(base, group)], rows, -1)
        offset = (rows & (BLK - 1)).astype(F32).astype(BF16)
        rows = jnp.transpose(rows, (1, 0))
        block = jnp.where(rows < 0, -1, lax.shift_right_arithmetic(rows, 7))
        second = jnp.where(block < 0, -1, block + blocks)
        for first in range(0, group, 16):
            key = jnp.concatenate([block[first : first + 8], second[first + 8 : first + 16]], axis=1)
            for k in range(8):
                n = first + k
                column = jnp.concatenate([offset[:, n : n + 1], offset[:, n + 8 : n + 9]], axis=0)
                in_block = jnp.where(key[k : k + 1] == block_order, 1.0, 0.0).astype(BF16)
                at_offset = jnp.where(column == offset_order, one, none)
                found = jnp.dot(in_block, at_offset, preferred_element_type=F32)
                staged[n * pitch : n * pitch + blocks, :] = found[:blocks]
                staged[(n + 8) * pitch : (n + 8) * pitch + blocks, :] = found[blocks:]
            for b in range(blocks):
                sixteen = staged[pl.ds(first * pitch + b, 16, stride=pitch), :].astype(BF16)
                counts_ref[b, pl.ds(pl.multiple_of(base + first, 16), 16), :] = sixteen
        return carry

    lax.fori_loop(0, share // group, some, 0)
    fetch_own.wait()
    fetch_ids.wait()
    held = [ids[0, s] for s in range(own.shape[0])]
    pooled_ref[...] = pooled_part(held, counts_ref, [own], split_rows)


def count_bags(rank, ids, index, length, own, share, blocks):
    bag = index.shape[0]
    hbm = pl.BlockSpec(memory_space=pltpu.HBM)
    return pl.pallas_call(
        count_kernel,
        in_specs=[pl.BlockSpec(memory_space=pltpu.SMEM)] + [hbm] * 4,
        out_specs=[pl.BlockSpec(memory_space=pltpu.VMEM)] * 2,
        out_shape=[
            pltpu.VMEM((blocks, share, BLK), BF16),
            pltpu.VMEM((share, own.shape[2]), F32),
        ],
        scratch_shapes=[
            pltpu.SMEM(ids.shape, jnp.int32),
            pltpu.VMEM((bag, share), jnp.int32),
            pltpu.VMEM((1, share), jnp.int32),
            pltpu.VMEM((256 * (blocks + 4), BLK), F32),
            pltpu.VMEM(own.shape, F32),
            pltpu.VMEM((own.shape[0] * BLK, 2 * own.shape[2]), BF16),
            pltpu.SemaphoreType.DMA((4,)),
        ],
        cost_estimate=pl.CostEstimate(
            flops=40 << 30, bytes_accessed=8388608, transcendentals=0
        ),
        compiler_params=pltpu.CompilerParams(vmem_limit_bytes=20 << 20),
        name="count_bags",
    )(rank, in_hbm(ids), in_hbm(index), in_hbm(length), in_hbm(own))


def pool_kernel(first_slot, has_prior, held_ref, counts_ref, *refs):
    refs = list(refs)
    split_rows = refs.pop()
    pooled_ref = refs.pop()
    prior_ref = refs.pop() if has_prior else None
    ids = [held_ref[first_slot + q] for q in range(len(refs) * refs[0].shape[0])]
    found = pooled_part(ids, counts_ref, refs, split_rows)
    pooled_ref[...] = found + prior_ref[...] if has_prior else found


def pool(held, first_slot, counts, parts, prior, keep):
    _, share, _ = counts.shape
    slots, _, width = parts[0].shape
    vmem = pl.BlockSpec(memory_space=pltpu.VMEM)
    arrays = [counts, *parts] + ([] if prior is None else [prior])
    return pl.pallas_call(
        functools.partial(pool_kernel, first_slot, prior is not None),
        in_specs=[pl.BlockSpec(memory_space=pltpu.SMEM)] + [vmem] * len(arrays),
        out_specs=vmem,
        out_shape=pltpu.VMEM((share, width), F32) if keep else pltpu.HBM((share, width), F32),
        scratch_shapes=[pltpu.VMEM((len(parts) * slots * BLK, 2 * width), BF16)],
        cost_estimate=pl.CostEstimate(
            flops=2 * share * len(parts) * slots * BLK * 2 * width,
            bytes_accessed=4 << 20,
            transcendentals=0,
        ),
        compiler_params=pltpu.CompilerParams(vmem_limit_bytes=24 << 20),
        name="pool",
    )(held, *[in_vmem(a) for a in arrays])


def move_kernel(held_ref, wanted_ref, part0, part1, part2, part3, moved_ref, target, sem):
    parts = (part0, part1, part2, part3)
    slots = part0.shape[0]
    for b in range(len(parts) * slots):
        target[b] = -1
    for s in range(slots):
        target[wanted_ref[s]] = s
    for k, part in enumerate(parts):
        for s in range(slots):
            goal = target[held_ref[k * slots + s]]

            @pl.when(goal >= 0)
            def _(part=part, s=s, goal=goal):
                pltpu.make_async_copy(part.at[s], moved_ref.at[goal], sem).start()

    pltpu.make_async_copy(part0, moved_ref, sem).wait()


def move_blocks(held, wanted, parts):
    slots, _, width = parts[0].shape
    smem = pl.BlockSpec(memory_space=pltpu.SMEM)
    hbm = pl.BlockSpec(memory_space=pltpu.HBM)
    return pl.pallas_call(
        move_kernel,
        in_specs=[smem, smem] + [pl.BlockSpec(memory_space=pltpu.VMEM)] * 4,
        out_specs=hbm,
        out_shape=jax.ShapeDtypeStruct((slots, BLK, width), F32),
        scratch_shapes=[pltpu.SMEM((len(parts) * slots,), jnp.int32), pltpu.SemaphoreType.DMA],
        compiler_params=pltpu.CompilerParams(vmem_limit_bytes=4 << 20),
        name="move_blocks",
    )(held, wanted, *[in_vmem(part) for part in parts])


def top_kernel(
    pooled_ref, dense_ref, first_hbm, second_hbm, out_ref, logits_ref,
    first_ref, second_ref, gram, joined, sems,
):
    samples, width = dense_ref.shape
    tables = pooled_ref.shape[0] // samples
    pitch = gram.shape[0] // samples
    inputs = first_ref.shape[0]
    depth = second_ref.shape[0]
    pieces = [(first_hbm, first_ref, at, min(FETCH, inputs - at)) for at in range(0, inputs, FETCH)]
    layer = len(pieces)
    pieces += [(second_hbm, second_ref, at, min(FETCH, depth - at)) for at in range(0, depth, FETCH)]
    fetches = [
        pltpu.make_async_copy(there.at[pl.ds(at, size)], here.at[pl.ds(at, size)], sems.at[k])
        for k, (there, here, at, size) in enumerate(pieces)
    ]
    for fetch in fetches:
        fetch.start()
    dense = dense_ref[...].astype(F32)
    for s in range(samples):
        top, rest = halves(pooled_ref[pl.ds(s, tables, stride=samples), :])
        own = jnp.broadcast_to(dense[s : s + 1], (8, width)).astype(BF16)
        none = jnp.zeros((8, width), BF16)
        tall_top = jnp.concatenate([top, own], axis=0)
        tall_rest = jnp.concatenate([rest, none], axis=0)
        left = jnp.concatenate([tall_top, tall_rest, tall_top], axis=1)
        right = jnp.concatenate([top, top, rest], axis=1)
        found = lax.dot_general(
            left, right, (((1,), (1,)), ((), ())), preferred_element_type=F32
        )
        gram[s * pitch : (s + 1) * pitch, :tables] = found * width ** (-0.5)
    lane = lax.broadcasted_iota(jnp.int32, (samples, 128), 1)
    joined[:, :width] = dense_ref[...]
    at = width
    filling = jnp.zeros((samples, 128), F32)
    for i in range(-1, tables - 1):
        row = tables if i < 0 else i
        start = 0 if i < 0 else i + 1
        line = gram[pl.ds(row, samples, stride=pitch), :]
        shift = (at - start) % 128
        line = pltpu.roll(line, shift, 1) if shift else line
        filling = jnp.where(lane >= at % 128, line, filling)
        after = at + tables - start
        if after // 128 != at // 128:
            base = at // 128 * 128
            joined[:, base : base + 128] = filling.astype(BF16)
            filling = line
        at = after
    base = at // 128 * 128
    if at % 128:
        joined[:, base : base + 128] = jnp.where(lane < at % 128, filling, 0.0).astype(BF16)
    hidden = jnp.zeros((samples, first_ref.shape[1]), F32)
    for fetch, (_, _, at, size) in zip(fetches[:layer], pieces[:layer]):
        fetch.wait()
        whole = size // 128 * 128
        for begin, count in ((at, whole), (at + whole, size - whole)):
            if count:
                ends = slice(begin, begin + count)
                hidden += jnp.dot(joined[:, ends], first_ref[ends], preferred_element_type=F32)
    value = jnp.maximum(hidden, 0.0).astype(BF16)
    hidden = jnp.zeros((samples, second_ref.shape[1]), F32)
    for fetch, (_, _, at, size) in zip(fetches[layer:], pieces[layer:]):
        fetch.wait()
        ends = slice(at, at + size)
        hidden += jnp.dot(value[:, ends], second_ref[ends], preferred_element_type=F32)
    hidden = jnp.maximum(hidden, 0.0).astype(BF16)
    last = jnp.broadcast_to(out_ref[...], (16, hidden.shape[1]))
    answer = lax.dot_general(last, hidden, (((1,), (1,)), ((), ())), preferred_element_type=F32)
    logits_ref[...] = answer[:1]


def top_of_model(pooled, dense, w_first, w_second, w_out):
    samples, _ = dense.shape
    tables = pooled.shape[0] // samples
    inputs, _ = w_first.shape
    padded = -(-inputs // 128) * 128
    hbm = pl.BlockSpec(memory_space=pltpu.HBM)
    vmem = pl.BlockSpec(memory_space=pltpu.VMEM)
    return pl.pallas_call(
        top_kernel,
        in_specs=[vmem, vmem, hbm, hbm, vmem],
        out_specs=vmem,
        out_shape=jax.ShapeDtypeStruct((1, samples), F32),
        scratch_shapes=[
            pltpu.VMEM(w_first.shape, BF16),
            pltpu.VMEM(w_second.shape, BF16),
            pltpu.VMEM((samples * (tables + 8), 128), F32),
            pltpu.VMEM((samples, padded), BF16),
            pltpu.SemaphoreType.DMA((-(-inputs // FETCH) - (-w_second.shape[0] // FETCH),)),
        ],
        compiler_params=pltpu.CompilerParams(vmem_limit_bytes=16 << 20),
        name="top_of_model",
    )(in_vmem(pooled), dense, in_hbm(w_first), in_hbm(w_second), w_out.reshape(1, -1))


def shards(
    old_table, old_blocks, new_blocks, bag_row_index, bag_length, dense, w_first, w_second, w_out
):
    slots = old_blocks.shape[1]
    width = old_table.shape[2]
    rows = lax.axis_size("row")
    rank = lax.axis_index("row")
    own = old_table[0].reshape(slots, BLK, width)
    other_core = [(k, k ^ 1) for k in range(rows)]
    other_chip = [(k, k ^ 2) for k in range(rows)]
    both = [(k, k ^ 3) for k in range(rows)]
    ids = old_blocks[0]
    across = lax.ppermute(own, "row", other_chip)
    beside = lax.ppermute(own, "row", other_core)
    named = [ids]
    for pairs in (other_core, other_chip, both):
        named.append(lax.ppermute(ids, "row", pairs))
    held = jnp.concatenate(named)
    share = bag_row_index.shape[0] // rows
    counts, pooled = count_bags(
        rank.astype(jnp.int32)[None],
        old_blocks,
        jnp.transpose(bag_row_index[:, 0, :]),
        jnp.transpose(bag_length),
        own,
        share,
        rows * slots,
    )
    far = lax.ppermute(across, "row", other_core)
    pooled = pool(held, slots, counts, (beside, across), pooled, True)
    pooled = pool(held, 3 * slots, counts, (far,), pooled, False)
    moved = move_blocks(held, new_blocks[0], (own, beside, across, far))
    cols = lax.axis_size("col")
    pooled = pooled.reshape(cols, share // cols, width)
    spread = lax.all_to_all(pooled, "col", split_axis=0, concat_axis=0, tiled=True)
    logits = top_of_model(spread.reshape(share, width), dense, w_first, w_second, w_out)
    return logits.reshape(-1), moved.reshape(1, slots * BLK, width)


def solution(mesh):
    in_specs = (
        P("col", "row", None),
        P("col", "row"),
        P("col", "row"),
        P(None, "col", None),
        P(None, "col"),
        P(("row", "col"), None),
        P(),
        P(),
        P(),
    )
    out_specs = (P(("row", "col")), P("col", "row", None))

    return jax.shard_map(shards, mesh=mesh, in_specs=in_specs, out_specs=out_specs, check_vma=False)
```

```python
import functools

import jax
import jax.numpy as jnp
from jax import lax
from jax.experimental import pallas as pl
from jax.experimental.pallas import tpu as pltpu
from jax.sharding import PartitionSpec as P


BLK = 128
FETCH = 256
BF16 = jnp.bfloat16
F32 = jnp.float32


def halves(x):
    top = x.astype(BF16)
    rest = (x - top.astype(F32)).astype(BF16)
    return top, rest


def in_vmem(x):
    return pltpu.with_memory_space_constraint(x, pltpu.VMEM)


def in_hbm(x):
    return pltpu.with_memory_space_constraint(x, pltpu.HBM)


def pooled_part(ids, counts_ref, parts, split_rows, chunk=None, take=None):
    slots, _, width = parts[0].shape
    for k, part in enumerate(parts):
        for s in range(slots):
            at = (k * slots + s) * BLK
            top, rest = halves(part[s])
            split_rows[at : at + BLK, :width] = top
            split_rows[at : at + BLK, width:] = rest
    share = counts_ref.shape[1]
    for m in range(0, share, chunk or share):
        ends = slice(m, m + (chunk or share))
        left = jnp.concatenate([counts_ref[b, ends] for b in ids], axis=1)
        found = jnp.dot(left, split_rows[...], preferred_element_type=F32)
        found = found[:, :width] + found[:, width:]
        if take is None:
            return found
        take(m, ends, found)


def count_kernel(
    rank_ref, ids_hbm, index_hbm, length_hbm, own_hbm, counts_ref, pooled_ref,
    ids, index, length, staged, own, split_rows, sems,
):
    bag, share = index.shape
    blocks = counts_ref.shape[0]
    group = 256
    pitch = staged.shape[0] // group
    start = pl.multiple_of(rank_ref[0] * share, 128)
    fetch_index = pltpu.make_async_copy(index_hbm.at[:, pl.ds(start, share)], index, sems.at[0])
    fetch_length = pltpu.make_async_copy(length_hbm.at[:, pl.ds(start, share)], length, sems.at[1])
    fetch_ids = pltpu.make_async_copy(ids_hbm, ids, sems.at[3])
    fetch_own = pltpu.make_async_copy(own_hbm, own, sems.at[2])
    fetch_index.start()
    fetch_length.start()
    fetch_own.start()
    fetch_ids.start()
    fetch_index.wait()
    fetch_length.wait()
    place = lax.broadcasted_iota(jnp.int32, (bag, group), 0)
    offset_order = lax.broadcasted_iota(jnp.int32, (2 * bag, BLK), 1).astype(F32).astype(BF16)
    block_order = lax.broadcasted_iota(jnp.int32, (2 * blocks, 2 * bag), 0)
    one = jnp.ones((), BF16)
    none = jnp.zeros((), BF16)

    def some(step, carry):
        base = pl.multiple_of(step * group, group)
        rows = index[:, pl.ds(base, group)]
        rows = jnp.where(place < length[:, pl.ds(base, group)], rows, -1)
        offset = (rows & (BLK - 1)).astype(F32).astype(BF16)
        rows = jnp.transpose(rows, (1, 0))
        block = jnp.where(rows < 0, -1, lax.shift_right_arithmetic(rows, 7))
        second = jnp.where(block < 0, -1, block + blocks)
        for first in range(0, group, 16):
            key = jnp.concatenate([block[first : first + 8], second[first + 8 : first + 16]], axis=1)
            for k in range(8):
                n = first + k
                column = jnp.concatenate([offset[:, n : n + 1], offset[:, n + 8 : n + 9]], axis=0)
                in_block = jnp.where(key[k : k + 1] == block_order, 1.0, 0.0).astype(BF16)
                at_offset = jnp.where(column == offset_order, one, none)
                found = jnp.dot(in_block, at_offset, preferred_element_type=F32)
                staged[n * pitch : n * pitch + blocks, :] = found[:blocks]
                staged[(n + 8) * pitch : (n + 8) * pitch + blocks, :] = found[blocks:]
            for b in range(blocks):
                sixteen = staged[pl.ds(first * pitch + b, 16, stride=pitch), :].astype(BF16)
                counts_ref[b, pl.ds(pl.multiple_of(base + first, 16), 16), :] = sixteen
        return carry

    lax.fori_loop(0, share // group, some, 0)
    fetch_own.wait()
    fetch_ids.wait()
    held = [ids[0, s] for s in range(own.shape[0])]
    pooled_ref[...] = pooled_part(held, counts_ref, [own], split_rows)


def count_bags(rank, ids, index, length, own, share, blocks):
    bag = index.shape[0]
    hbm = pl.BlockSpec(memory_space=pltpu.HBM)
    return pl.pallas_call(
        count_kernel,
        in_specs=[pl.BlockSpec(memory_space=pltpu.SMEM)] + [hbm] * 4,
        out_specs=[pl.BlockSpec(memory_space=pltpu.VMEM)] * 2,
        out_shape=[
            pltpu.VMEM((blocks, share, BLK), BF16),
            pltpu.VMEM((share, own.shape[2]), F32),
        ],
        scratch_shapes=[
            pltpu.SMEM(ids.shape, jnp.int32),
            pltpu.VMEM((bag, share), jnp.int32),
            pltpu.VMEM((1, share), jnp.int32),
            pltpu.VMEM((256 * (blocks + 4), BLK), F32),
            pltpu.VMEM(own.shape, F32),
            pltpu.VMEM((own.shape[0] * BLK, 2 * own.shape[2]), BF16),
            pltpu.SemaphoreType.DMA((4,)),
        ],
        cost_estimate=pl.CostEstimate(
            flops=40 << 30, bytes_accessed=8388608, transcendentals=0
        ),
        compiler_params=pltpu.CompilerParams(vmem_limit_bytes=20 << 20),
        name="count_bags",
    )(rank, in_hbm(ids), in_hbm(index), in_hbm(length), in_hbm(own))


def pool_kernel(first_slot, has_prior, keep, held_ref, counts_ref, *refs):
    refs = list(refs)
    sems, sums = (None, None) if keep else (refs.pop(), refs.pop())
    split_rows = refs.pop()
    pooled_ref = refs.pop()
    prior_ref = refs.pop() if has_prior else None
    ids = [held_ref[first_slot + q] for q in range(len(refs) * refs[0].shape[0])]
    if keep:
        found = pooled_part(ids, counts_ref, refs, split_rows)
        pooled_ref[...] = found + prior_ref[...] if has_prior else found
        return
    chunk = pooled_ref.shape[0] // 2
    sent = []

    def send(m, ends, found):
        sums[ends] = found + prior_ref[ends] if has_prior else found
        rows = pl.ds(m, chunk)
        out = pltpu.make_async_copy(sums.at[rows], pooled_ref.at[rows], sems.at[m // chunk])
        out.start()
        sent.append(out)

    pooled_part(ids, counts_ref, refs, split_rows, chunk, send)
    for out in sent:
        out.wait()


def pool(held, first_slot, counts, parts, prior, keep):
    _, share, _ = counts.shape
    slots, _, width = parts[0].shape
    vmem = pl.BlockSpec(memory_space=pltpu.VMEM)
    arrays = [counts, *parts] + ([] if prior is None else [prior])
    return pl.pallas_call(
        functools.partial(pool_kernel, first_slot, prior is not None, keep),
        in_specs=[pl.BlockSpec(memory_space=pltpu.SMEM)] + [vmem] * len(arrays),
        out_specs=vmem if keep else pl.BlockSpec(memory_space=pltpu.HBM),
        out_shape=pltpu.VMEM((share, width), F32) if keep else pltpu.HBM((share, width), F32),
        scratch_shapes=[pltpu.VMEM((len(parts) * slots * BLK, 2 * width), BF16)]
        + ([] if keep else [pltpu.VMEM((share, width), F32), pltpu.SemaphoreType.DMA((2,))]),
        cost_estimate=pl.CostEstimate(
            flops=2 * share * len(parts) * slots * BLK * 2 * width,
            bytes_accessed=4 << 20,
            transcendentals=0,
        ),
        compiler_params=pltpu.CompilerParams(vmem_limit_bytes=24 << 20),
        name="pool",
    )(held, *[in_vmem(a) for a in arrays])


def move_kernel(held_ref, wanted_ref, part0, part1, part2, part3, moved_ref, target, sem):
    parts = (part0, part1, part2, part3)
    slots = part0.shape[0]
    for b in range(len(parts) * slots):
        target[b] = -1
    for s in range(slots):
        target[wanted_ref[s]] = s
    for k, part in enumerate(parts):
        for s in range(slots):
            goal = target[held_ref[k * slots + s]]

            @pl.when(goal >= 0)
            def _(part=part, s=s, goal=goal):
                pltpu.make_async_copy(part.at[s], moved_ref.at[goal], sem).start()

    pltpu.make_async_copy(part0, moved_ref, sem).wait()


def move_blocks(held, wanted, parts):
    slots, _, width = parts[0].shape
    smem = pl.BlockSpec(memory_space=pltpu.SMEM)
    hbm = pl.BlockSpec(memory_space=pltpu.HBM)
    return pl.pallas_call(
        move_kernel,
        in_specs=[smem, smem] + [pl.BlockSpec(memory_space=pltpu.VMEM)] * 4,
        out_specs=hbm,
        out_shape=jax.ShapeDtypeStruct((slots, BLK, width), F32),
        scratch_shapes=[pltpu.SMEM((len(parts) * slots,), jnp.int32), pltpu.SemaphoreType.DMA],
        compiler_params=pltpu.CompilerParams(vmem_limit_bytes=4 << 20),
        name="move_blocks",
    )(held, wanted, *[in_vmem(part) for part in parts])


def top_kernel(
    pooled_ref, dense_ref, first_hbm, second_hbm, out_ref, logits_ref,
    first_ref, second_ref, gram, joined, sems,
):
    samples, width = dense_ref.shape
    tables = pooled_ref.shape[0] // samples
    pitch = gram.shape[0] // samples
    inputs = first_ref.shape[0]
    depth = second_ref.shape[0]
    pieces = [(first_hbm, first_ref, at, min(FETCH, inputs - at)) for at in range(0, inputs, FETCH)]
    layer = len(pieces)
    pieces += [(second_hbm, second_ref, at, min(FETCH, depth - at)) for at in range(0, depth, FETCH)]
    fetches = [
        pltpu.make_async_copy(there.at[pl.ds(at, size)], here.at[pl.ds(at, size)], sems.at[k])
        for k, (there, here, at, size) in enumerate(pieces)
    ]
    for fetch in fetches:
        fetch.start()
    dense = dense_ref[...].astype(F32)
    for s in range(samples):
        top, rest = halves(pooled_ref[pl.ds(s, tables, stride=samples), :])
        own = jnp.broadcast_to(dense[s : s + 1], (8, width)).astype(BF16)
        none = jnp.zeros((8, width), BF16)
        tall_top = jnp.concatenate([top, own], axis=0)
        tall_rest = jnp.concatenate([rest, none], axis=0)
        left = jnp.concatenate([tall_top, tall_rest, tall_top], axis=1)
        right = jnp.concatenate([top, top, rest], axis=1)
        found = lax.dot_general(
            left, right, (((1,), (1,)), ((), ())), preferred_element_type=F32
        )
        gram[s * pitch : (s + 1) * pitch, :tables] = found * width ** (-0.5)
    lane = lax.broadcasted_iota(jnp.int32, (samples, 128), 1)
    joined[:, :width] = dense_ref[...]
    at = width
    filling = jnp.zeros((samples, 128), F32)
    for i in range(-1, tables - 1):
        row = tables if i < 0 else i
        start = 0 if i < 0 else i + 1
        line = gram[pl.ds(row, samples, stride=pitch), :]
        shift = (at - start) % 128
        line = pltpu.roll(line, shift, 1) if shift else line
        filling = jnp.where(lane >= at % 128, line, filling)
        after = at + tables - start
        if after // 128 != at // 128:
            base = at // 128 * 128
            joined[:, base : base + 128] = filling.astype(BF16)
            filling = line
        at = after
    base = at // 128 * 128
    if at % 128:
        joined[:, base : base + 128] = jnp.where(lane < at % 128, filling, 0.0).astype(BF16)
    hidden = jnp.zeros((samples, first_ref.shape[1]), F32)
    for fetch, (_, _, at, size) in zip(fetches[:layer], pieces[:layer]):
        fetch.wait()
        whole = size // 128 * 128
        for begin, count in ((at, whole), (at + whole, size - whole)):
            if count:
                ends = slice(begin, begin + count)
                hidden += jnp.dot(joined[:, ends], first_ref[ends], preferred_element_type=F32)
    value = jnp.maximum(hidden, 0.0).astype(BF16)
    hidden = jnp.zeros((samples, second_ref.shape[1]), F32)
    for fetch, (_, _, at, size) in zip(fetches[layer:], pieces[layer:]):
        fetch.wait()
        ends = slice(at, at + size)
        hidden += jnp.dot(value[:, ends], second_ref[ends], preferred_element_type=F32)
    hidden = jnp.maximum(hidden, 0.0).astype(BF16)
    last = jnp.broadcast_to(out_ref[...], (16, hidden.shape[1]))
    answer = lax.dot_general(last, hidden, (((1,), (1,)), ((), ())), preferred_element_type=F32)
    logits_ref[...] = answer[:1]


def top_of_model(pooled, dense, w_first, w_second, w_out):
    samples, _ = dense.shape
    tables = pooled.shape[0] // samples
    inputs, _ = w_first.shape
    padded = -(-inputs // 128) * 128
    hbm = pl.BlockSpec(memory_space=pltpu.HBM)
    vmem = pl.BlockSpec(memory_space=pltpu.VMEM)
    return pl.pallas_call(
        top_kernel,
        in_specs=[vmem, vmem, hbm, hbm, vmem],
        out_specs=vmem,
        out_shape=jax.ShapeDtypeStruct((1, samples), F32),
        scratch_shapes=[
            pltpu.VMEM(w_first.shape, BF16),
            pltpu.VMEM(w_second.shape, BF16),
            pltpu.VMEM((samples * (tables + 8), 128), F32),
            pltpu.VMEM((samples, padded), BF16),
            pltpu.SemaphoreType.DMA((-(-inputs // FETCH) - (-w_second.shape[0] // FETCH),)),
        ],
        compiler_params=pltpu.CompilerParams(vmem_limit_bytes=16 << 20),
        name="top_of_model",
    )(in_vmem(pooled), dense, in_hbm(w_first), in_hbm(w_second), w_out.reshape(1, -1))


def shards(
    old_table, old_blocks, new_blocks, bag_row_index, bag_length, dense, w_first, w_second, w_out
):
    slots = old_blocks.shape[1]
    width = old_table.shape[2]
    rows = lax.axis_size("row")
    rank = lax.axis_index("row")
    own = old_table[0].reshape(slots, BLK, width)
    other_core = [(k, k ^ 1) for k in range(rows)]
    other_chip = [(k, k ^ 2) for k in range(rows)]
    both = [(k, k ^ 3) for k in range(rows)]
    ids = old_blocks[0]
    across = lax.ppermute(own, "row", other_chip)
    beside = lax.ppermute(own, "row", other_core)
    named = [ids]
    for pairs in (other_core, other_chip, both):
        named.append(lax.ppermute(ids, "row", pairs))
    held = jnp.concatenate(named)
    share = bag_row_index.shape[0] // rows
    counts, pooled = count_bags(
        rank.astype(jnp.int32)[None],
        old_blocks,
        jnp.transpose(bag_row_index[:, 0, :]),
        jnp.transpose(bag_length),
        own,
        share,
        rows * slots,
    )
    far = lax.ppermute(across, "row", other_core)
    pooled = pool(held, slots, counts, (beside, across), pooled, True)
    pooled = pool(held, 3 * slots, counts, (far,), pooled, False)
    moved = move_blocks(held, new_blocks[0], (own, beside, across, far))
    cols = lax.axis_size("col")
    pooled = pooled.reshape(cols, share // cols, width)
    spread = lax.all_to_all(pooled, "col", split_axis=0, concat_axis=0, tiled=True)
    logits = top_of_model(spread.reshape(share, width), dense, w_first, w_second, w_out)
    return logits.reshape(-1), moved.reshape(1, slots * BLK, width)


def solution(mesh):
    in_specs = (
        P("col", "row", None),
        P("col", "row"),
        P("col", "row"),
        P(None, "col", None),
        P(None, "col"),
        P(("row", "col"), None),
        P(),
        P(),
        P(),
    )
    out_specs = (P(("row", "col")), P("col", "row", None))

    return jax.shard_map(shards, mesh=mesh, in_specs=in_specs, out_specs=out_specs, check_vma=False)
```
